32 devices in a mesh: seq: 16 (over z, y, x), head: 2 (over core).
Axes of the slice: x: 2, y: 2, z: 4, core: 2. Of those that a mesh axis runs over, the one named last changes fastest.
Arguments:
- hidden_in: bfloat16 [4, 16384], P(None, 'seq'), may hold values from -12 to 12
- norm_gain: float32 [16384], P('seq'), may hold values from 0.25 to 1.75
- qkv_codes: int32 [16384, 4608], P('seq', 'head'), may hold values from 0 to 255
- qkv_scale: float32 [18432], P('head'), may hold values from 0.00390625 to 0.015625
- out_codes: int32 [16384, 4096], P('seq', 'head'), may hold values from 0 to 255
- out_scale: float32 [16384], P('seq'), may hold values from 0.0078125 to 0.03125
- cache_keys: bfloat16 [4, 16384, 8, 128], P(None, 'seq', 'head'), may hold values from -200 to 200
- cache_values: bfloat16 [4, 16384, 8, 128], P(None, 'seq', 'head'), may hold values from -6 to 6
- lengths: int32 [4], replicated, may hold values from 8192 to 16384, as said below
Outputs:
- hidden_out: bfloat16 [4, 16384], P(None, 'seq')
The draws below stay inside these ranges and needn't reach their ends.
Inputs may be any that keep to these rules, and one draw needn't show every extreme that they name: `lengths`: some sequence uses all 16384 cached positions in every draw.
All inputs are finite; a program needn't handle non-finite values.
Results may differ from the reference program's by a relative error of at most 0.02.
The reference program's roundings to bfloat16 on the way (of `w_qkv`, `w_out`, `normed`, `queries`, `weights` and `attended`) count: a program that leaves them out, or rounds other values in their place, can miss the bound.
Values sent between devices are 32-bit elements; how exact they have to be, the bound alone decides.
A program may use at most 192 MiB of HBM per device.

```python
import math
import jax
import jax.numpy as jnp
import numpy as np
from jax import lax

D = 16384
HEADS = 128
KV_HEADS = 8
HEAD_DIM = 128
TILE = 128
DECODE_STEPS = 2
BATCH = 4
CACHE_DEV = 1024
CACHE_LEN = 16384


def draw_hidden_in(key, part):
    places = jnp.arange(D, dtype=jnp.float32) / D
    ramp_scale = 0.6 + 1.2 * places
    values = jax.random.truncated_normal(key, -6.0, 6.0, (BATCH, D), jnp.float32)
    return (values * ramp_scale[None, :]).astype(jnp.bfloat16)


def draw_cache_keys(key, part):
    full_shape = (BATCH, CACHE_LEN, KV_HEADS, HEAD_DIM)
    values = 2.5 * jax.random.truncated_normal(key, -6.0, 6.0, full_shape, jnp.float32)
    return values.astype(jnp.bfloat16)


def draw_lengths(key, part):
    base_draw = jax.random.randint(jax.random.fold_in(key, 31), (BATCH,), CACHE_LEN // 2, CACHE_LEN)
    chosen_row = jax.random.randint(jax.random.fold_in(key, 32), (), 0, BATCH)
    return jnp.where(jnp.arange(BATCH) == chosen_row, CACHE_LEN, base_draw).astype(jnp.int32)


def with_ends(result, rng, smallest, largest):
    place = [jax.random.randint(jax.random.fold_in(rng, axis), (), 0, length) for axis, length in enumerate(result.shape)]
    widest = result.shape.index(max(result.shape))
    beside = place[:widest] + [(place[widest] + 1) % result.shape[widest]] + place[widest + 1:]
    return result.at[tuple(place)].set(smallest).at[tuple(beside)].set(largest)


def block_levels(key, shape, cuts, least, high):
    gain, own = 1.0, jax.random.fold_in(key, 6)
    for position, blocks in cuts:
        draws = jnp.exp(jax.random.uniform(jax.random.fold_in(own, position), (blocks,), jnp.float32, least / len(cuts), high / len(cuts)))
        gain = gain * jnp.repeat(draws, shape[position] // blocks).reshape([-1 if axis == position else 1 for axis in range(len(shape))])
    return gain


def centred(stream_key, extent, width, bound, shards=(), kind=jnp.bfloat16):
    values = jax.random.normal(stream_key, extent, jnp.float32) * width
    if len(shards) > 0:
        values = block_levels(stream_key, extent, shards, -0.22, 0.18) * values
    return jnp.clip(values, min=-bound, max=bound).astype(kind)


def setup_inputs(seed: int = 0) -> dict:
    keys = jax.random.split(jax.random.key(seed), 10)
    return {
        "hidden_in": draw_hidden_in(jax.random.fold_in(keys[9], 71), 0),
        "norm_gain": jnp.clip(1.0 + 0.15 * jax.random.normal(keys[1], (D,), jnp.float32), 0.25, 1.75),
        "qkv_codes": with_ends(jax.random.randint(keys[2], (D, KV_HEADS * (HEADS // KV_HEADS + 2) * HEAD_DIM // 4), 0, 256), jax.random.fold_in(keys[2], 1), 0, 255).astype(jnp.int32),
        "qkv_scale": jnp.clip(jnp.exp(math.log(0.015625) - 1.3862944 * jax.random.uniform(keys[3], (KV_HEADS * (HEADS // KV_HEADS + 2) * HEAD_DIM,), jnp.float32) ** block_levels(keys[3], (KV_HEADS * (HEADS // KV_HEADS + 2) * HEAD_DIM,), ((0, 2),), -0.2, 0.2)), 0.00390625, 0.015625),
        "out_codes": with_ends(jax.random.randint(keys[4], (D, HEADS * HEAD_DIM // 4), 0, 256), jax.random.fold_in(keys[4], 1), 0, 255).astype(jnp.int32),
        "out_scale": jnp.clip(jnp.exp(math.log(0.03125) - 1.3862944 * jax.random.uniform(keys[5], (D,), jnp.float32) ** block_levels(keys[5], (D,), ((0, 16),), -0.2, 0.2)), 0.0078125, 0.03125),
        "cache_keys": draw_cache_keys(jax.random.fold_in(keys[9], 71), 0),
        "cache_values": centred(keys[7], (BATCH, CACHE_LEN, KV_HEADS, HEAD_DIM), 1.0, 6.0, ((1, 16), (2, 2))),
        "lengths": draw_lengths(jax.random.fold_in(keys[9], 71), 0),
    }


code_norm = 147.8
epsilon = 1e-05
rope_base = 500000.0

def decode_codes(code_words):
    num_rows = code_words.shape[0]
    tile_bytes = TILE // 4
    byte_tiles = code_words.reshape(num_rows, -1, tile_bytes)
    byte_first = jnp.repeat(byte_tiles, 4, axis=2)
    byte_second = jnp.repeat(jnp.roll(byte_tiles, -1, axis=2), 4, axis=2)
    byte_third = jnp.repeat(jnp.roll(byte_tiles, -2, axis=2), 4, axis=2)
    window = byte_first * 65536 + byte_second * 256 + byte_third
    divisor = jnp.asarray(np.array([256, 64, 16, 4])[np.arange(TILE) % 4], dtype=jnp.int32)
    trellis_state = window // divisor % 65536
    low_product = trellis_state * 25297 + 13946
    low_half = low_product % 65536
    high_half = (trellis_state * 519 + 1169 + low_product // 65536) % 65536
    byte_total = low_half % 256 + low_half // 256 + high_half % 256 + high_half // 256
    return ((byte_total - 510).astype(jnp.float32) / code_norm).reshape(num_rows, -1)

def rope_tables(positions):
    half_dim = HEAD_DIM // 2
    freqs = jnp.exp(-(jnp.arange(half_dim, dtype=jnp.float32) * (2.0 / HEAD_DIM)) * math.log(rope_base))
    angles = positions.astype(jnp.float32)[:, None] * freqs[None, :]
    return (jnp.cos(angles), jnp.sin(angles))

def rotate(values, cosine_table, sine_table):
    half_dim = values.shape[-1] // 2
    first_half = values[..., :half_dim]
    second = values[..., half_dim:]
    return jnp.concatenate([first_half * cosine_table - second * sine_table, second * cosine_table + first_half * sine_table], axis=-1)

def finish(top_max, denominator, numerator, queries, new_keys, new_values):
    score_scale = HEAD_DIM ** (-0.5)
    query_float = queries.astype(jnp.float32)
    new_scores = [lax.optimization_barrier(jnp.sum(query_float * new_key.astype(jnp.float32)[:, :, None, :], axis=-1)) * score_scale for new_key in new_keys]
    peak_score = top_max
    for new_score in new_scores:
        peak_score = jnp.maximum(peak_score, new_score)
    factor = jnp.exp(top_max - peak_score)
    denominator = denominator * factor
    numerator = numerator * factor[..., None]
    for new_score, new_value in zip(new_scores, new_values):
        weight_new = jnp.exp(new_score - peak_score)
        denominator = denominator + weight_new
        numerator = numerator + weight_new[..., None] * new_value.astype(jnp.float32)[:, :, None, :]
    attended = numerator / denominator[..., None]
    return attended.astype(jnp.bfloat16).reshape(attended.shape[0], -1)

def cache_part(queries, cache_keys, cache_values, lengths):
    score_scale = HEAD_DIM ** (-0.5)
    blocks = CACHE_LEN // CACHE_DEV
    live_mask = (jnp.arange(CACHE_LEN, dtype=jnp.int32)[None, :] < lengths[:, None]).reshape(BATCH, 1, blocks, CACHE_DEV)

    def one_head(operands):
        head_query, head_keys, head_values = operands
        scores = jnp.einsum('brd,bld->brl', head_query.astype(jnp.float32), head_keys.astype(jnp.float32)) * score_scale
        scores = scores.reshape(BATCH, -1, blocks, CACHE_DEV)
        block_max = lax.optimization_barrier(jnp.max(jnp.where(live_mask, scores, -1e+30), axis=3))
        weights = jnp.where(live_mask, jnp.exp(scores - block_max[..., None]), 0.0)
        block_sum = lax.optimization_barrier(jnp.sum(weights, axis=3))
        rounded = lax.optimization_barrier(weights.astype(jnp.bfloat16)).astype(jnp.float32)
        block_values = head_values.astype(jnp.float32).reshape(BATCH, blocks, CACHE_DEV, HEAD_DIM)
        block_acc = jnp.einsum('brnc,bncd->brnd', rounded, block_values)
        top_max = lax.optimization_barrier(jnp.max(block_max, axis=2))
        factor = jnp.exp(block_max - top_max[..., None])
        return (top_max, lax.optimization_barrier(jnp.sum(block_sum * factor, axis=2)), lax.optimization_barrier(jnp.sum(block_acc * factor[..., None], axis=2)))
    stacked = lax.map(one_head, (jnp.moveaxis(queries, 1, 0), jnp.moveaxis(cache_keys, 2, 0), jnp.moveaxis(cache_values, 2, 0)))
    return tuple((jnp.moveaxis(member, 0, 1) for member in stacked))

def reference(hidden_in, norm_gain, qkv_codes, qkv_scale, out_codes, out_scale, cache_keys, cache_values, lengths):
    row_block = math.gcd(D, 512)

    def decode_qkv(code_block):
        return (decode_codes(code_block) * qkv_scale[None, :]).astype(jnp.bfloat16)

    def decode_out(operands):
        code_block, scale_block = operands
        return (decode_codes(code_block) * scale_block[:, None]).astype(jnp.bfloat16)
    w_qkv = lax.map(decode_qkv, qkv_codes.reshape(D // row_block, row_block, -1)).reshape(D, -1)
    w_out = lax.map(decode_out, (out_codes.reshape(D // row_block, row_block, -1), out_scale.reshape(D // row_block, row_block))).reshape(D, -1)
    groups = HEADS // KV_HEADS
    hidden = hidden_in
    new_keys = []
    new_values = []
    for decode_step in range(DECODE_STEPS):
        positions = lengths + decode_step
        squares = lax.optimization_barrier(jnp.sum(jnp.square(hidden.astype(jnp.float32)), axis=1))
        normed = (hidden.astype(jnp.float32) * norm_gain[None, :]).astype(jnp.bfloat16)
        projected = jnp.dot(normed, w_qkv, preferred_element_type=jnp.float32)
        projected = projected * lax.rsqrt(squares / D + epsilon)[:, None]
        grouped = projected.reshape(BATCH, KV_HEADS, groups + 2, HEAD_DIM)
        cosine_table, sine_table = rope_tables(positions)
        queries = rotate(grouped[:, :, :groups], cosine_table[:, None, None, :], sine_table[:, None, None, :]).astype(jnp.bfloat16)
        new_keys.append(rotate(grouped[:, :, groups], cosine_table[:, None, :], sine_table[:, None, :]).astype(jnp.bfloat16))
        new_values.append(grouped[:, :, groups + 1].astype(jnp.bfloat16))
        top_max, denominator, numerator = cache_part(queries, cache_keys, cache_values, lengths)
        attended = finish(top_max, denominator, numerator, queries, new_keys, new_values)
        update = lax.dot_general(attended, w_out, (((1,), (1,)), ((), ())), preferred_element_type=jnp.float32)
        hidden = (hidden.astype(jnp.float32) + update).astype(jnp.bfloat16)
    return hidden
```

```python
import functools
import math

import jax
import jax.numpy as jnp
from jax import lax
from jax.experimental import pallas as pl
from jax.experimental.pallas import tpu as pltpu
from jax.sharding import PartitionSpec as P

HEADS = 128
KV_HEADS = 8
HEAD_DIM = 128
TILE = 128
DECODE_STEPS = 2

code_norm = 147.8
epsilon = 1e-05
rope_base = 500000.0

LANES = 128
WIDE = 4 * LANES
GROUP = HEADS // KV_HEADS
PER_KV = GROUP + 2
TILE_BYTES = TILE // 4
ROWS = 128
DEPTH = 3
BYTES = 0x00FF00FF
LOW = -1e30
MESH = pl.DeviceIdType.MESH
NT = (((1,), (1,)), ((), ()))


def byte_windows(first):
    lane = lax.broadcasted_iota(jnp.int32, first.shape, 1)
    base = lane & ~(TILE_BYTES - 1)
    one = base | ((lane + 1) & (TILE_BYTES - 1))
    two = base | ((lane + 2) & (TILE_BYTES - 1))
    second = jnp.take_along_axis(first, one, axis=1)
    third = jnp.take_along_axis(first, two, axis=1)
    return (((first << 8) | second) << 8) | third


def hashed_weight(window, phase):
    state = lax.shift_right_logical(window, 8 - 2 * phase)
    if phase:
        state = state & 65535
    hashed = state * 34038481 + 76625530
    halves = (hashed & BYTES) + (lax.shift_right_logical(hashed, 8) & BYTES)
    total = lax.shift_right_logical(halves * 65537, 16) - 510
    return total.astype(jnp.float32).astype(jnp.bfloat16)


class Stream:
    def __init__(self, codes, buf, win, sem, weights):
        self.codes, self.buf, self.win, self.sem, self.weights = codes, buf, win, sem, weights
        self.count = codes.shape[1] // LANES
        self.rows = codes.shape[0]
        self.block = math.gcd(ROWS, self.rows)
        self.steps = self.rows // self.block

    def copy(self, chunk):
        slot = lax.rem(chunk, DEPTH)
        column = pl.multiple_of(chunk * LANES, LANES)
        return pltpu.make_async_copy(
            self.codes.at[:, pl.ds(column, LANES)], self.buf.at[slot], self.sem.at[slot]
        )

    def begin(self):
        for chunk in range(min(DEPTH, self.count)):
            self.copy(chunk).start()

    def block_rows(self, step):
        return pl.ds(pl.multiple_of(step * self.block, self.block), self.block)

    def first_windows(self):
        self.copy(0).wait()

        def body(step, carry):
            rows = self.block_rows(step)
            self.win[0, rows, :] = byte_windows(self.buf[0, rows, :])
            return carry

        lax.fori_loop(0, self.steps, body, 0)

    def chunk(self, chunk, beside=None):
        now, later = lax.rem(chunk, 2), lax.rem(chunk + 1, 2)
        slot = lax.rem(chunk + 1, DEPTH)

        @pl.when(chunk + 1 < self.count)
        def _():
            self.copy(chunk + 1).wait()

        @pl.when(chunk + DEPTH < self.count)
        def _():
            self.copy(chunk + DEPTH).start()

        def body(step, carry):
            rows = self.block_rows(step)
            if beside is not None:
                beside(chunk, step, rows)
            window = self.win[now, rows, :]
            for phase in range(4):
                self.weights[chunk, phase, rows, :] = hashed_weight(window, phase)
            self.win[later, rows, :] = byte_windows(self.buf[slot, rows, :])
            return carry

        lax.fori_loop(0, self.steps, body, 0)

    def run(self, low, high):
        def body(chunk, carry):
            self.chunk(chunk)
            return carry

        if high > low:
            lax.fori_loop(low, high, body, 0)


def kernel(
    hidden_ref,
    gain_ref,
    qkv_codes,
    qkv_scale,
    out_codes,
    out_scale,
    keys_hbm,
    values_hbm,
    lengths,
    cosine,
    sine,
    out_ref,
    w_qkv,
    w_out,
    qkv_buf,
    qkv_win,
    out_buf,
    out_win,
    keys,
    values,
    perm,
    padded,
    normed,
    hidden,
    accum,
    part,
    stage,
    owned_scale,
    square_all,
    arrived,
    heads_all,
    scores,
    merge_send,
    merge_arrived,
    attended,
    attended_own,
    by_phase,
    share,
    share_arrived,
    qkv_sem,
    out_sem,
    cache_sem,
    square_send_sem,
    square_sem,
    part_send_sem,
    part_sem,
    heads_send_sem,
    heads_sem,
    merge_send_sem,
    merge_sem,
    attended_send_sem,
    attended_sem,
    share_send_sem,
    share_sem,
):
    count = lax.axis_size("seq")
    head_count = lax.axis_size("head")
    me = lax.axis_index("seq")
    head = lax.axis_index("head")
    batch, depth = hidden_ref.shape
    features = depth * count
    chunks = w_qkv.shape[0]
    out_chunks = w_out.shape[0]
    owners = -(-chunks // count)
    cached = keys.shape[1]
    head_rows = attended.shape[1]
    groups = head_rows // GROUP
    block_len = cached // groups
    rows_each = merge_send.shape[1] - 1
    score_scale = HEAD_DIM ** (-0.5)

    def peer(step):
        return lax.rem(me + step, count)

    qkv = Stream(qkv_codes, qkv_buf, qkv_win, qkv_sem, w_qkv)
    outs = Stream(out_codes, out_buf, out_win, out_sem, w_out)
    qkv.begin()
    barrier = pltpu.get_barrier_semaphore()
    for step in range(1, count):
        pl.semaphore_signal(barrier, inc=1, device_id=(peer(step), head), device_id_type=MESH)
    for step in range(1, head_count):
        other = lax.rem(head + step, head_count)
        pl.semaphore_signal(barrier, inc=1, device_id=(me, other), device_id_type=MESH)

    def build(step, carry):
        rows = pl.ds(pl.multiple_of(step * LANES, LANES), LANES)
        natural = lax.broadcasted_iota(jnp.int32, (LANES, WIDE), 0) + step * LANES
        lane = lax.broadcasted_iota(jnp.int32, (LANES, WIDE), 1)
        source = ((lane >> 5) & 3) * LANES + (lane & 31) * 4 + (lane >> 7)
        perm[rows, :] = jnp.where(natural == source, 1.0, 0.0).astype(jnp.bfloat16)
        return carry

    lax.fori_loop(0, 4, build, 0)
    stage[...] = jnp.zeros_like(stage)
    padded[...] = jnp.zeros_like(padded)
    attended[...] = jnp.zeros_like(attended)
    hidden[...] = hidden_ref[...].astype(jnp.float32)

    for index in range(owners):
        chunk = jnp.minimum(me + index * count, chunks - 1)
        column = pl.multiple_of(chunk * WIDE, WIDE)
        scale = qkv_scale[0:1, pl.ds(column, WIDE)] / code_norm
        high = scale.astype(jnp.bfloat16).astype(jnp.float32)
        middle = (scale - high).astype(jnp.bfloat16).astype(jnp.float32)
        low = scale - high - middle
        stage[0:1, :] = high
        stage[1:2, :] = middle
        stage[2:3, :] = low
        moved = jnp.dot(
            stage[...].astype(jnp.bfloat16), perm[...], preferred_element_type=jnp.float32
        )
        owned_scale[index] = jnp.broadcast_to(
            moved[0:1, :] + moved[1:2, :] + moved[2:3, :], (8, WIDE)
        )
    stage[...] = jnp.zeros_like(stage)

    def start_square_copies(step_index):
        for step in range(1, count):
            pltpu.make_async_remote_copy(
                src_ref=square_all.at[step_index, 0],
                dst_ref=square_all.at[step_index, step],
                send_sem=square_send_sem.at[step_index, step],
                recv_sem=square_sem.at[step_index, step],
                device_id=(peer(step), head),
                device_id_type=MESH,
            ).start()

    def square_copy(step_index, step):
        return pltpu.make_async_remote_copy(
            src_ref=square_all.at[step_index, 0],
            dst_ref=square_all.at[step_index, step],
            send_sem=square_send_sem.at[step_index, step],
            recv_sem=square_sem.at[step_index, step],
            device_id=(peer(step), head),
            device_id_type=MESH,
        )

    def begin_step(step_index):
        values_now = hidden[...]
        squares = jnp.sum(jnp.square(values_now), axis=1, keepdims=True)
        square_all[step_index, 0] = jnp.broadcast_to(squares, (batch, LANES))
        padded[0:batch, :] = values_now * gain_ref[...]
        normed[...] = padded[...].astype(jnp.bfloat16)

    def part_copy(step_index, chunk):
        owner = lax.rem(chunk, count)
        index = chunk // count
        offset = lax.rem(owner - me + count, count)
        return pltpu.make_async_remote_copy(
            src_ref=part.at[step_index, chunk],
            dst_ref=arrived.at[step_index, index, jnp.maximum(offset - 1, 0)],
            send_sem=part_send_sem.at[step_index, chunk],
            recv_sem=part_sem.at[step_index, index],
            device_id=(owner, head),
            device_id_type=MESH,
        )

    def send_part(step_index, chunk):
        @pl.when(lax.rem(chunk, count) != me)
        def _():
            part_copy(step_index, chunk).start()

    def qkv_product(chunk):
        weights = jnp.concatenate([w_qkv[chunk, phase] for phase in range(4)], axis=1)
        return jnp.dot(normed[...], weights, preferred_element_type=jnp.float32)

    def heads_copy(step_index, chunk, step):
        rows = pl.ds(pl.multiple_of(chunk * 16, 16), 16)
        return pltpu.make_async_remote_copy(
            src_ref=heads_all.at[step_index, rows, :],
            dst_ref=heads_all.at[step_index, rows, :],
            send_sem=heads_send_sem.at[step_index, chunk // count, step],
            recv_sem=heads_sem.at[step_index, chunk],
            device_id=(peer(step), head),
            device_id_type=MESH,
        )

    def finish_heads(step_index):
        for step in range(1, count):
            square_copy(step_index, step).wait_recv()
        squares = square_all[step_index, 0]
        for step in range(1, count):
            squares = squares + square_all[step_index, step]
        inverse = lax.rsqrt(squares / features + epsilon)
        lane = lax.broadcasted_iota(jnp.int32, (8, LANES), 1)
        lower = (lane & 31) < 16
        for index in range(owners):
            chunk = me + index * count

            def work(index=index, chunk=chunk):
                pieces = arrived.at[step_index, index]
                pltpu.make_async_copy(pieces, pieces, part_sem.at[step_index, index]).wait()
                total = part[step_index, chunk]
                for step in range(count - 1):
                    total = total + arrived[step_index, index, step]
                first = lax.rem(4 * chunk, PER_KV)
                place = first + (lane >> 5)
                place = jnp.where(place >= PER_KV, place - PER_KV, place)
                plain = place == PER_KV - 1
                for phase in range(4):
                    columns = slice(phase * LANES, (phase + 1) * LANES)
                    padded_inverse = inverse
                    stage[0:batch, columns] = total[:, columns] * padded_inverse
                    entry = stage[0:8, columns] * owned_scale[index, :, columns]
                    partner = jnp.where(
                        lower, pltpu.roll(entry, LANES - 16, 1), pltpu.roll(entry, 16, 1)
                    )
                    turned = (
                        entry * cosine[step_index, phase] + partner * sine[step_index, phase]
                    )
                    stage[0:8, columns] = jnp.where(plain, entry, turned)
                natural = lax.dot_general(
                    stage[...].astype(jnp.bfloat16),
                    perm[...],
                    NT,
                    preferred_element_type=jnp.float32,
                )
                for place_in in range(4):
                    accum[place_in * 4 : place_in * 4 + 4, 0:LANES] = natural[
                        0:4, place_in * LANES : (place_in + 1) * LANES
                    ]
                rows = pl.ds(pl.multiple_of(chunk * 16, 16), 16)
                heads_all[step_index, rows, :] = accum[:, 0:LANES]
                for step in range(1, count):
                    heads_copy(step_index, chunk, step).start()

            if (index + 1) * count <= chunks:
                work()
            else:
                pl.when(chunk < chunks)(work)

    def wait_heads(step_index):
        for chunk in range(chunks):

            @pl.when(me != chunk % count)
            def _(chunk=chunk):
                heads_copy(step_index, chunk, 1).wait_recv()

    def merge_copy(step_index, step):
        target = peer(step)
        return pltpu.make_async_remote_copy(
            src_ref=merge_send.at[step_index * count + target],
            dst_ref=merge_arrived.at[step_index, step],
            send_sem=merge_send_sem.at[step_index, step],
            recv_sem=merge_sem.at[step_index, step],
            device_id=(target, head),
            device_id_type=MESH,
        )

    def attend(step_index):
        wait_heads(step_index)
        column = lax.broadcasted_iota(jnp.int32, (head_rows, cached), 1)
        row = lax.broadcasted_iota(jnp.int32, (head_rows, cached), 0)
        if step_index == 0:
            for b in range(batch):
                pltpu.make_async_copy(keys_hbm.at[b], keys.at[b], cache_sem.at[0, b]).wait()
                pltpu.make_async_copy(values_hbm.at[b], values.at[b], cache_sem.at[1, b]).wait()
        width = math.gcd(cached, 1024)
        tiles = cached // width
        lane = lax.broadcasted_iota(jnp.int32, (head_rows, LANES), 1)
        line = lax.broadcasted_iota(jnp.int32, (head_rows, LANES), 0)
        for b in range(batch):
            query = jnp.concatenate(
                [
                    heads_all[step_index, pl.ds(g * PER_KV * 4 + b, GROUP, stride=4), :]
                    for g in range(groups)
                ],
                axis=0,
            ).astype(jnp.bfloat16)
            live_length = lengths[b] - me * block_len
            top = jnp.full((head_rows, 1), LOW, jnp.float32)
            for tile in range(tiles):
                columns = slice(tile * width, (tile + 1) * width)
                score = (
                    lax.dot_general(
                        query, keys[b, columns, :], NT, preferred_element_type=jnp.float32
                    )
                    * score_scale
                )
                position = lax.broadcasted_iota(jnp.int32, (head_rows, width), 1) + tile * width
                row_group = lax.broadcasted_iota(jnp.int32, (head_rows, width), 0) // GROUP
                live = position < live_length * groups
                if groups > 1:
                    live = live & (lax.rem(position, groups) == row_group)
                score = jnp.where(live, score, LOW)
                scores[b % 2, :, columns] = score
                top = jnp.maximum(top, jnp.max(score, axis=1, keepdims=True))
            total = jnp.zeros((head_rows, 1), jnp.float32)
            mixed = jnp.zeros((head_rows, HEAD_DIM), jnp.float32)
            for tile in range(tiles):
                columns = slice(tile * width, (tile + 1) * width)
                score = scores[b % 2, :, columns]
                weight = jnp.where(score > 0.5 * LOW, jnp.exp(score - top), 0.0)
                total = total + jnp.sum(weight, axis=1, keepdims=True)
                mixed = mixed + jnp.dot(
                    weight.astype(jnp.bfloat16),
                    values[b, columns, :],
                    preferred_element_type=jnp.float32,
                )
            spread = jnp.where(lane == line, top, 0.0) + jnp.where(
                lane == line + LANES // 2, total, 0.0
            )
            spread = jnp.sum(spread, axis=0, keepdims=True)
            each = head_rows // rows_each
            for piece in range(each):
                slot = step_index * count + b * each + piece
                merge_send[slot, 0:rows_each, :] = mixed[
                    piece * rows_each : (piece + 1) * rows_each, :
                ]
                merge_send[slot, rows_each : rows_each + 1, :] = spread
        for step in range(1, count):
            merge_copy(step_index, step).start()

    def attended_place():
        first = me * rows_each
        b = first // head_rows
        line = lax.rem(first, head_rows)
        return b, line

    def attended_copy(step_index, step):
        b, line = attended_place()
        return pltpu.make_async_remote_copy(
            src_ref=attended_own.at[step_index],
            dst_ref=attended.at[step_index, pl.ds(line, rows_each), b, :],
            send_sem=attended_send_sem.at[step_index, step],
            recv_sem=attended_sem.at[step_index],
            device_id=(peer(step), head),
            device_id_type=MESH,
        )

    def merge(step_index):
        for step in range(1, count):
            merge_copy(step_index, step).wait_recv()
        b, line = attended_place()
        own = step_index * count + me
        pieces = [merge_send[own, 0:rows_each, :]]
        stats = [merge_send[own, rows_each : rows_each + 1, :]]
        for step in range(1, count):
            pieces.append(merge_arrived[step_index, step, 0:rows_each, :])
            stats.append(merge_arrived[step_index, step, rows_each : rows_each + 1, :])
        top = stats[0]
        for stat in stats[1:]:
            top = jnp.maximum(top, stat)
        lane = lax.broadcasted_iota(jnp.int32, (rows_each, LANES), 1)
        row = lax.broadcasted_iota(jnp.int32, (rows_each, LANES), 0)
        chosen = lane == line + row

        def to_column(values_row):
            spread = jnp.where(chosen, jnp.broadcast_to(values_row, (rows_each, LANES)), 0.0)
            return jnp.sum(spread, axis=1, keepdims=True)

        upper = lax.broadcasted_iota(jnp.int32, (1, LANES), 1) < LANES // 2
        numerator = jnp.zeros((rows_each, HEAD_DIM), jnp.float32)
        denominator_row = jnp.zeros((1, LANES), jnp.float32)
        for piece, stat in zip(pieces, stats):
            factor = jnp.exp(jnp.where(upper, stat - top, LOW))
            numerator = numerator + piece * to_column(factor)
            sums = jnp.concatenate([stat[:, LANES // 2 :], stat[:, : LANES // 2]], axis=1)
            denominator_row = denominator_row + sums * factor
        top_column = to_column(top)
        denominator = to_column(denominator_row)
        group = line // GROUP
        start = (group * PER_KV + lax.rem(line, GROUP)) * 4 + b
        query = heads_all[step_index, pl.ds(start, rows_each, stride=4), :]
        new_at = (group * PER_KV + GROUP) * 4 + b
        new_scores = []
        new_values = []
        for past in range(step_index + 1):
            new_key = heads_all[past, pl.ds(new_at, 1), :]
            new_values.append(heads_all[past, pl.ds(new_at + 4, 1), :])
            new_scores.append(jnp.sum(query * new_key, axis=1, keepdims=True) * score_scale)
        peak = top_column
        for new_score in new_scores:
            peak = jnp.maximum(peak, new_score)
        factor = jnp.exp(top_column - peak)
        denominator = denominator * factor
        numerator = numerator * factor
        for new_score, new_value in zip(new_scores, new_values):
            weight = jnp.exp(new_score - peak)
            denominator = denominator + weight
            numerator = numerator + weight * new_value
        attended_own[step_index] = numerator / denominator
        for step in range(1, count):
            attended_copy(step_index, step).start()
        for place in range(rows_each):
            attended[step_index, line + place, pl.ds(b, 1), :] = attended_own[
                step_index, place : place + 1, :
            ]

    def share_copy(step_index, step):
        other = lax.rem(head + step, head_count)
        return pltpu.make_async_remote_copy(
            src_ref=share.at[step_index],
            dst_ref=share_arrived.at[step_index, head],
            send_sem=share_send_sem.at[step_index, step],
            recv_sem=share_sem.at[step_index, step],
            device_id=(me, other),
            device_id_type=MESH,
        )

    def project(step_index):
        others = arrived_attended(step_index)
        others.wait()
        lines = jnp.concatenate(
            [
                attended[step_index, pl.ds(place, out_chunks, stride=4), :, :].reshape(
                    out_chunks * 8, LANES
                )
                for place in range(4)
            ],
            axis=1,
        ).astype(jnp.bfloat16)
        moved = jnp.dot(lines, perm[...], preferred_element_type=jnp.float32)
        by_phase[...] = moved.reshape(out_chunks, 8, WIDE)

        def body(chunk, total):
            weights = jnp.concatenate([w_out[chunk, phase] for phase in range(4)], axis=1)
            return total + lax.dot_general(
                by_phase[chunk].astype(jnp.bfloat16),
                weights,
                NT,
                preferred_element_type=jnp.float32,
            )

        total = lax.fori_loop(0, out_chunks, body, jnp.zeros((8, depth), jnp.float32))
        scaled = total[0:batch, :] * (out_scale[...] / code_norm)
        share[step_index] = scaled
        share_arrived[step_index, head] = scaled
        for step in range(1, head_count):
            share_copy(step_index, step).start()
        for step in range(1, head_count):
            share_copy(step_index, step).wait_recv()
        update = share_arrived[step_index, 0]
        for other in range(1, head_count):
            update = update + share_arrived[step_index, other]
        fresh = (hidden[...] + update).astype(jnp.bfloat16)
        hidden[...] = fresh.astype(jnp.float32)

    def arrived_attended(step_index):
        class Waiter:
            def wait(self):
                spread = merge_arrived.at[step_index, pl.ds(1, count - 1), 0:rows_each, :]
                pltpu.make_async_copy(spread, spread, attended_sem.at[step_index]).wait()

        return Waiter()

    begin_step(0)
    qkv.first_windows()
    outs.begin()
    for b in range(batch):
        pltpu.make_async_copy(keys_hbm.at[b], keys.at[b], cache_sem.at[0, b]).start()
        pltpu.make_async_copy(values_hbm.at[b], values.at[b], cache_sem.at[1, b]).start()
    pl.semaphore_wait(barrier, count - 1 + head_count - 1)
    for step in range(1, count):
        square_copy(0, step).start()

    def beside(chunk, step, rows):
        before = jnp.maximum(chunk - 1, 0)
        weights = jnp.concatenate([w_qkv[before, phase, rows, :] for phase in range(4)], axis=1)
        product = jnp.dot(normed[:, rows], weights, preferred_element_type=jnp.float32)
        accum[...] += product

    def qkv_step(chunk, carry):
        accum[...] = jnp.zeros_like(accum)
        qkv.chunk(chunk, beside)
        part[0, chunk - 1] = accum[0:batch, :]
        send_part(0, chunk - 1)
        return carry

    qkv.chunk(0)
    lax.fori_loop(1, chunks, qkv_step, 0)
    part[0, chunks - 1] = qkv_product(chunks - 1)[0:batch, :]
    send_part(0, chunks - 1)
    marks = [0, out_chunks * 5 // 16, out_chunks * 10 // 16, out_chunks * 13 // 16, out_chunks]
    outs.first_windows()
    outs.run(marks[0], marks[1])
    finish_heads(0)
    outs.run(marks[1], marks[2])
    attend(0)
    outs.run(marks[2], marks[3])
    merge(0)
    outs.run(marks[3], marks[4])
    project(0)

    for step_index in range(1, DECODE_STEPS):
        begin_step(step_index)
        for step in range(1, count):
            square_copy(step_index, step).start()

        def again(chunk, carry):
            part[step_index, chunk] = qkv_product(chunk)[0:batch, :]
            send_part(step_index, chunk)
            return carry

        lax.fori_loop(0, chunks, again, 0)
        finish_heads(step_index)
        attend(step_index)
        merge(step_index)
        project(step_index)

    out_ref[...] = hidden[...].astype(jnp.bfloat16)

    for step_index in range(DECODE_STEPS):
        for step in range(1, count):
            square_copy(step_index, step).wait_send()
            merge_copy(step_index, step).wait_send()
            attended_copy(step_index, step).wait_send()
        for step in range(1, head_count):
            share_copy(step_index, step).wait_send()
        for chunk in range(chunks):

            @pl.when(me != chunk % count)
            def _(chunk=chunk):
                part_copy(step_index, chunk).wait_send()

            @pl.when(me == chunk % count)
            def _(chunk=chunk):
                for step in range(1, count):
                    heads_copy(step_index, chunk, step).wait_send()


def padded_codes(codes):
    extra = -codes.shape[1] % LANES
    return jnp.pad(codes, ((0, 0), (0, extra))) if extra else codes


def rope_tables(lengths):
    half = HEAD_DIM // 2
    lane = jnp.arange(LANES, dtype=jnp.int32) % TILE_BYTES
    phase = jnp.arange(4, dtype=jnp.int32)
    entry = 4 * lane[None, :] + phase[:, None]
    freqs = jnp.exp(
        -((entry % half).astype(jnp.float32) * (2.0 / HEAD_DIM)) * math.log(rope_base)
    )
    steps = jnp.arange(DECODE_STEPS, dtype=jnp.int32)
    positions = (lengths[None, :] + steps[:, None]).astype(jnp.float32)
    angles = positions[:, None, :, None] * freqs[None, :, None, :]
    sign = jnp.where(entry < half, -1.0, 1.0)[None, :, None, :]
    rows = ((0, 0), (0, 0), (0, 8 - lengths.shape[0]), (0, 0))
    return jnp.pad(jnp.cos(angles), rows), jnp.pad(jnp.sin(angles) * sign, rows)


def shards(
    hidden_in,
    norm_gain,
    qkv_codes,
    qkv_scale,
    out_codes,
    out_scale,
    cache_keys,
    cache_values,
    lengths,
):
    count = lax.axis_size("seq")
    head_count = lax.axis_size("head")
    batch, depth = hidden_in.shape
    qkv_codes = padded_codes(qkv_codes)
    out_codes = padded_codes(out_codes)
    chunks = qkv_codes.shape[1] // LANES
    out_chunks = out_codes.shape[1] // LANES
    extra = chunks * WIDE - qkv_scale.shape[0]
    if extra:
        qkv_scale = jnp.pad(qkv_scale, (0, extra))
    groups = cache_keys.shape[2]
    cached = cache_keys.shape[1] * groups
    head_rows = groups * GROUP
    rows_each = batch * head_rows // count
    owners = -(-chunks // count)
    cosine, sine = rope_tables(lengths)
    f32, bf16 = jnp.float32, jnp.bfloat16
    vmem = pl.BlockSpec(memory_space=pltpu.VMEM)
    hbm = pl.BlockSpec(memory_space=pl.ANY)
    steps = DECODE_STEPS
    dma = pltpu.SemaphoreType.DMA
    return pl.pallas_call(
        kernel,
        in_specs=[
            vmem, vmem, hbm, vmem, hbm, vmem, hbm, hbm,
            pl.BlockSpec(memory_space=pltpu.SMEM), vmem, vmem,
        ],
        out_specs=vmem,
        out_shape=jax.ShapeDtypeStruct((batch, depth), bf16),
        scratch_shapes=[
            pltpu.VMEM((chunks, 4, depth, LANES), bf16),
            pltpu.VMEM((out_chunks, 4, depth, LANES), bf16),
            pltpu.VMEM((DEPTH, depth, LANES), jnp.int32),
            pltpu.VMEM((2, depth, LANES), jnp.int32),
            pltpu.VMEM((DEPTH, depth, LANES), jnp.int32),
            pltpu.VMEM((2, depth, LANES), jnp.int32),
            pltpu.VMEM((batch, cached, HEAD_DIM), bf16),
            pltpu.VMEM((batch, cached, HEAD_DIM), bf16),
            pltpu.VMEM((WIDE, WIDE), bf16),
            pltpu.VMEM((16, depth), f32),
            pltpu.VMEM((16, depth), bf16),
            pltpu.VMEM((batch, depth), f32),
            pltpu.VMEM((16, WIDE), f32),
            pltpu.VMEM((steps, chunks, batch, WIDE), f32),
            pltpu.VMEM((16, WIDE), f32),
            pltpu.VMEM((owners, 8, WIDE), f32),
            pltpu.VMEM((steps, count, batch, LANES), f32),
            pltpu.VMEM((steps, owners, count - 1, batch, WIDE), f32),
            pltpu.VMEM((steps, chunks * 16, LANES), f32),
            pltpu.VMEM((2, head_rows, cached), f32),
            pltpu.VMEM((steps * count, rows_each + 1, LANES), f32),
            pltpu.VMEM((steps, count, rows_each + 1, LANES), f32),
            pltpu.VMEM((steps, head_rows, 8, LANES), f32),
            pltpu.VMEM((steps, rows_each, LANES), f32),
            pltpu.VMEM((out_chunks, 8, WIDE), f32),
            pltpu.VMEM((steps, batch, depth), f32),
            pltpu.VMEM((steps, head_count, batch, depth), f32),
            dma((DEPTH,)),
            dma((DEPTH,)),
            dma((2, batch)),
            dma((steps, count)),
            dma((steps, count)),
            dma((steps, chunks)),
            dma((steps, owners)),
            dma((steps, owners, count)),
            dma((steps, chunks)),
            dma((steps, count)),
            dma((steps, count)),
            dma((steps, count)),
            dma((steps,)),
            dma((steps, head_count)),
            dma((steps, head_count)),
        ],
        compiler_params=pltpu.CompilerParams(
            collective_id=0, has_side_effects=True, vmem_limit_bytes=66_000_000
        ),
    )(
        hidden_in,
        norm_gain[None, :],
        qkv_codes,
        qkv_scale[None, :],
        out_codes,
        out_scale[None, :],
        cache_keys.reshape(batch, cached, HEAD_DIM),
        cache_values.reshape(batch, cached, HEAD_DIM),
        lengths,
        cosine,
        sine,
    )


def solution(mesh):
    in_specs = (
        P(None, "seq"),
        P("seq"),
        P("seq", "head"),
        P("head"),
        P("seq", "head"),
        P("seq"),
        P(None, "seq", "head", None),
        P(None, "seq", "head", None),
        P(),
    )
    out_specs = P(None, "seq")
    return jax.shard_map(shards, mesh=mesh, in_specs=in_specs, out_specs=out_specs, check_vma=False)
```

```python
import functools
import math

import jax
import jax.numpy as jnp
from jax import lax
from jax.experimental import pallas as pl
from jax.experimental.pallas import tpu as pltpu
from jax.sharding import PartitionSpec as P

HEADS = 128
KV_HEADS = 8
HEAD_DIM = 128
TILE = 128
DECODE_STEPS = 2

code_norm = 147.8
epsilon = 1e-05
rope_base = 500000.0

LANES = 128
WIDE = 4 * LANES
GROUP = HEADS // KV_HEADS
PER_KV = GROUP + 2
TILE_BYTES = TILE // 4
ROWS = 256
SMALL = 128
DEPTH = 4
BYTES = 0x00FF00FF
LOW = -1e30
MESH = pl.DeviceIdType.MESH
NT = (((1,), (1,)), ((), ()))


def window_matrix(turned):
    row = lax.broadcasted_iota(jnp.int32, (LANES, LANES), 0)
    lane = lax.broadcasted_iota(jnp.int32, (LANES, LANES), 1)
    source, place = (lane, row) if turned else (row, lane)
    base = place & ~(TILE_BYTES - 1)
    one = base | ((place + 1) & (TILE_BYTES - 1))
    two = base | ((place + 2) & (TILE_BYTES - 1))
    matrix = jnp.where(source == place, 65536.0, 0.0)
    matrix = matrix + jnp.where(source == one, 256.0, 0.0)
    return (matrix + jnp.where(source == two, 1.0, 0.0)).astype(jnp.bfloat16)


def hashed_weight(window, phase):
    state = lax.shift_right_logical(window, 8 - 2 * phase)
    if phase:
        state = state & 65535
    hashed = state * 34038481 + 76625530
    halves = (hashed & BYTES) + (lax.shift_right_logical(hashed, 8) & BYTES)
    total = lax.shift_right_logical(halves * 65537, 16) - 510
    return total.astype(jnp.float32).astype(jnp.bfloat16)


class Stream:
    def __init__(self, codes, buf, win, sem, weights, matrix):
        self.matrix = matrix
        self.codes, self.buf, self.win, self.sem, self.weights = codes, buf, win, sem, weights
        self.count = codes.shape[1] // LANES
        self.rows = codes.shape[0]
        self.block = math.gcd(ROWS, self.rows)
        self.steps = self.rows // self.block

    def copy(self, chunk):
        slot = lax.rem(chunk, DEPTH)
        column = pl.multiple_of(chunk * LANES, LANES)
        return pltpu.make_async_copy(
            self.codes.at[:, pl.ds(column, LANES)], self.buf.at[slot], self.sem.at[slot]
        )

    def begin(self):
        for chunk in range(min(DEPTH, self.count)):
            self.copy(chunk).start()

    def block_rows(self, step):
        return pl.ds(pl.multiple_of(step * self.block, self.block), self.block)

    def first_windows(self):
        self.copy(0).wait()

        def body(step, carry):
            self.form(0, 0, step)
            return carry

        lax.fori_loop(0, self.steps, body, 0)

    def form(self, slot, place, step):
        rows = self.block_rows(step)
        codes = self.buf[slot, rows, :].astype(jnp.float32).astype(jnp.bfloat16)
        window = jnp.dot(codes, self.matrix[...], preferred_element_type=jnp.float32)
        self.win[place, rows, :] = window.astype(jnp.int32)

    def hash(self, chunk, place, step):
        small = math.gcd(self.block, SMALL)
        for part in range(self.block // small):
            rows = pl.ds(pl.multiple_of(step * self.block + part * small, small), small)
            window = self.win[place, rows, :]
            for phase in range(4):
                self.weights[chunk, phase, rows, :] = hashed_weight(window, phase)

    def chunk(self, chunk, beside=None):
        now, later = lax.rem(chunk, 2), lax.rem(chunk + 1, 2)
        slot = lax.rem(chunk + 1, DEPTH)

        @pl.when(chunk + 1 < self.count)
        def _():
            self.copy(chunk + 1).wait()

        @pl.when(chunk + DEPTH < self.count)
        def _():
            self.copy(chunk + DEPTH).start()

        def body(step, carry):
            if beside is not None:
                beside(chunk, step, self.block_rows(step))
            self.hash(chunk, now, step)
            self.form(slot, later, step)
            return carry

        lax.fori_loop(0, self.steps, body, 0)

    def run(self, low, high):
        def body(chunk, carry):
            self.chunk(chunk)
            return carry

        if high > low:
            lax.fori_loop(low, high, body, 0)


class TurnedStream(Stream):
    def blocks(self, step):
        for place in range(self.block // LANES):
            yield step * (self.block // LANES) + place

    def form(self, slot, place, step):
        for block in self.blocks(step):
            rows = pl.ds(pl.multiple_of(block * LANES, LANES), LANES)
            codes = self.buf[slot, rows, :].astype(jnp.float32).astype(jnp.bfloat16)
            window = lax.dot_general(
                self.matrix[...], codes, NT, preferred_element_type=jnp.float32
            )
            self.win[place, rows, :] = window.astype(jnp.int32)

    def hash(self, chunk, place, step):
        for block in self.blocks(step):
            for part in range(0, LANES, SMALL):
                rows = pl.ds(pl.multiple_of(block * LANES + part, SMALL), SMALL)
                window = self.win[place, rows, :]
                for phase in range(4):
                    lines = slice(phase * LANES + part, phase * LANES + part + SMALL)
                    self.weights[chunk, block, lines, :] = hashed_weight(window, phase)


def kernel(
    hidden_ref,
    gain_ref,
    qkv_codes,
    qkv_scale,
    out_codes,
    out_scale,
    keys_hbm,
    values_hbm,
    lengths,
    out_ref,
    w_qkv,
    w_out,
    qkv_buf,
    qkv_win,
    out_buf,
    out_win,
    keys,
    values,
    cosine,
    sine,
    perm,
    windows,
    padded,
    normed,
    hidden,
    accum,
    part,
    stage,
    owned_scale,
    square_all,
    arrived,
    heads_all,
    scores,
    merge_send,
    merge_arrived,
    attended,
    attended_own,
    by_phase,
    share,
    share_arrived,
    qkv_sem,
    out_sem,
    cache_sem,
    square_send_sem,
    square_sem,
    part_send_sem,
    part_sem,
    heads_send_sem,
    heads_sem,
    merge_send_sem,
    merge_sem,
    attended_send_sem,
    attended_sem,
    share_send_sem,
    share_sem,
):
    count = lax.axis_size("seq")
    head_count = lax.axis_size("head")
    me = lax.axis_index("seq")
    head = lax.axis_index("head")
    batch, depth = hidden_ref.shape
    features = depth * count
    chunks = w_qkv.shape[0]
    out_chunks = w_out.shape[0]
    owners = -(-chunks // count)
    cached = keys.shape[1]
    head_rows = attended.shape[1]
    groups = head_rows // GROUP
    block_len = cached // groups
    rows_each = merge_send.shape[1] - 1
    score_scale = HEAD_DIM ** (-0.5)

    def peer(step):
        return lax.rem(me + step, count)

    def wait_bytes(ref, sem):
        pltpu.make_async_copy(ref, ref, sem).wait()

    qkv = Stream(qkv_codes, qkv_buf, qkv_win, qkv_sem, w_qkv, windows.at[0])
    outs = TurnedStream(out_codes, out_buf, out_win, out_sem, w_out, windows.at[1])
    qkv.begin()
    windows[0] = window_matrix(False)
    windows[1] = window_matrix(True)
    barrier = pltpu.get_barrier_semaphore()
    for step in range(1, count):
        pl.semaphore_signal(barrier, inc=1, device_id=(peer(step), head), device_id_type=MESH)
    for step in range(1, head_count):
        other = lax.rem(head + step, head_count)
        pl.semaphore_signal(barrier, inc=1, device_id=(me, other), device_id_type=MESH)

    def build(step, carry):
        rows = pl.ds(pl.multiple_of(step * LANES, LANES), LANES)
        natural = lax.broadcasted_iota(jnp.int32, (LANES, WIDE), 0) + step * LANES
        lane = lax.broadcasted_iota(jnp.int32, (LANES, WIDE), 1)
        source = ((lane >> 5) & 3) * LANES + (lane & 31) * 4 + (lane >> 7)
        perm[rows, :] = jnp.where(natural == source, 1.0, 0.0).astype(jnp.bfloat16)
        return carry

    lax.fori_loop(0, 4, build, 0)
    stage[...] = jnp.zeros_like(stage)
    padded[...] = jnp.zeros_like(padded)
    attended[...] = jnp.zeros_like(attended)
    hidden[...] = hidden_ref[...].astype(jnp.float32)

    for step in range(DECODE_STEPS):
        for phase in range(4):
            tables = rope_tables(lengths, batch, step, phase)
            cosine[step, phase], sine[step, phase] = tables

    for index in range(owners):
        chunk = jnp.minimum(me + index * count, chunks - 1)
        column = pl.multiple_of(chunk * WIDE, WIDE)
        scale = qkv_scale[0:1, pl.ds(column, WIDE)] / code_norm
        high = scale.astype(jnp.bfloat16).astype(jnp.float32)
        middle = (scale - high).astype(jnp.bfloat16).astype(jnp.float32)
        low = scale - high - middle
        stage[0:1, :] = high
        stage[1:2, :] = middle
        stage[2:3, :] = low
        moved = jnp.dot(
            stage[...].astype(jnp.bfloat16), perm[...], preferred_element_type=jnp.float32
        )
        owned_scale[index] = jnp.broadcast_to(
            moved[0:1, :] + moved[1:2, :] + moved[2:3, :], (8, WIDE)
        )
    stage[...] = jnp.zeros_like(stage)

    def square_copy(step_index, step):
        return pltpu.make_async_remote_copy(
            src_ref=square_all.at[step_index, 0],
            dst_ref=square_all.at[step_index, step],
            send_sem=square_send_sem.at[step_index],
            recv_sem=square_sem.at[step_index],
            device_id=(peer(step), head),
            device_id_type=MESH,
        )

    def begin_step(step_index):
        values_now = hidden[...]
        squares = jnp.sum(jnp.square(values_now), axis=1, keepdims=True)
        square_all[step_index, 0] = jnp.broadcast_to(squares, (batch, LANES))
        padded[0:batch, :] = values_now * gain_ref[...]
        normed[...] = padded[...].astype(jnp.bfloat16)

    def part_copy(step_index, chunk):
        owner = lax.rem(chunk, count)
        index = chunk // count
        offset = lax.rem(owner - me + count, count)
        return pltpu.make_async_remote_copy(
            src_ref=part.at[step_index, chunk],
            dst_ref=arrived.at[step_index, index, jnp.maximum(offset - 1, 0)],
            send_sem=part_send_sem.at[step_index],
            recv_sem=part_sem.at[step_index, index],
            device_id=(owner, head),
            device_id_type=MESH,
        )

    def send_part(step_index, chunk):
        @pl.when(lax.rem(chunk, count) != me)
        def _():
            part_copy(step_index, chunk).start()

    def qkv_product(chunk):
        weights = jnp.concatenate([w_qkv[chunk, phase] for phase in range(4)], axis=1)
        return jnp.dot(normed[...], weights, preferred_element_type=jnp.float32)

    def heads_copy(step_index, chunk, step):
        rows = pl.ds(pl.multiple_of(chunk * 16, 16), 16)
        return pltpu.make_async_remote_copy(
            src_ref=heads_all.at[step_index, rows, :],
            dst_ref=heads_all.at[step_index, rows, :],
            send_sem=heads_send_sem.at[step_index, chunk // count],
            recv_sem=heads_sem.at[step_index],
            device_id=(peer(step), head),
            device_id_type=MESH,
        )

    def finish_heads(step_index):
        wait_bytes(square_all.at[step_index, pl.ds(1, count - 1)], square_sem.at[step_index])
        squares = square_all[step_index, 0]
        for step in range(1, count):
            squares = squares + square_all[step_index, step]
        inverse = lax.rsqrt(squares / features + epsilon)
        lane = lax.broadcasted_iota(jnp.int32, (8, LANES), 1)
        lower = (lane & 31) < 16
        for index in range(owners):
            chunk = me + index * count

            def work(index=index, chunk=chunk):
                wait_bytes(arrived.at[step_index, index], part_sem.at[step_index, index])
                total = part[step_index, chunk]
                for step in range(count - 1):
                    total = total + arrived[step_index, index, step]
                first = lax.rem(4 * chunk, PER_KV)
                place = first + (lane >> 5)
                place = jnp.where(place >= PER_KV, place - PER_KV, place)
                plain = place == PER_KV - 1
                for phase in range(4):
                    columns = slice(phase * LANES, (phase + 1) * LANES)
                    padded_inverse = inverse
                    stage[0:batch, columns] = total[:, columns] * padded_inverse
                    entry = stage[0:8, columns] * owned_scale[index, :, columns]
                    partner = jnp.where(
                        lower, pltpu.roll(entry, LANES - 16, 1), pltpu.roll(entry, 16, 1)
                    )
                    turned = (
                        entry * cosine[step_index, phase] + partner * sine[step_index, phase]
                    )
                    stage[0:8, columns] = jnp.where(plain, entry, turned)
                natural = lax.dot_general(
                    stage[...].astype(jnp.bfloat16),
                    perm[...],
                    NT,
                    preferred_element_type=jnp.float32,
                )
                for place_in in range(4):
                    accum[place_in * 4 : place_in * 4 + 4, 0:LANES] = natural[
                        0:4, place_in * LANES : (place_in + 1) * LANES
                    ]
                rows = pl.ds(pl.multiple_of(chunk * 16, 16), 16)
                heads_all[step_index, rows, :] = accum[:, 0:LANES]
                for step in range(1, count):
                    heads_copy(step_index, chunk, step).start()

            if (index + 1) * count <= chunks:
                work()
            else:
                pl.when(chunk < chunks)(work)

    def by_owned(action):
        least = chunks // count
        if chunks % count == 0:
            action(least)
        else:

            @pl.when(me < chunks % count)
            def _():
                action(least + 1)

            @pl.when(me >= chunks % count)
            def _():
                action(least)

    def wait_heads(step_index):
        def action(owned):
            if chunks > owned:
                rows = pl.ds(0, (chunks - owned) * 16)
                wait_bytes(heads_all.at[step_index, rows, :], heads_sem.at[step_index])

        by_owned(action)

    def wait_part_sends(step_index):
        def action(owned):
            if chunks > owned:
                sent = part.at[step_index, pl.ds(0, chunks - owned)]
                wait_bytes(sent, part_send_sem.at[step_index])
            for index in range(owned):
                wait_bytes(arrived.at[step_index, index], heads_send_sem.at[step_index, index])

        by_owned(action)

    def merge_copy(step_index, step):
        target = peer(step)
        return pltpu.make_async_remote_copy(
            src_ref=merge_send.at[step_index * count + target],
            dst_ref=merge_arrived.at[step_index, step],
            send_sem=merge_send_sem.at[step_index],
            recv_sem=merge_sem.at[step_index],
            device_id=(target, head),
            device_id_type=MESH,
        )

    def attend(step_index):
        wait_heads(step_index)
        if step_index == 0:
            for b in range(batch):
                pltpu.make_async_copy(keys_hbm.at[b], keys.at[b], cache_sem.at[0, b]).wait()
                pltpu.make_async_copy(values_hbm.at[b], values.at[b], cache_sem.at[1, b]).wait()
        width = math.gcd(cached, 1024)
        tiles = cached // width
        lane = lax.broadcasted_iota(jnp.int32, (head_rows, LANES), 1)
        line = lax.broadcasted_iota(jnp.int32, (head_rows, LANES), 0)
        power = score_scale * math.log2(math.e)
        blank = jnp.zeros((head_rows, HEAD_DIM), jnp.float32)

        def over_lanes(block, combine):
            result = block[:, :LANES]
            for start in range(LANES, width, LANES):
                result = combine(result, block[:, start : start + LANES])
            return result

        def mask(b, tile):
            position = lax.broadcasted_iota(jnp.int32, (8, width), 1) + tile * width
            live = position < (lengths[b] - me * block_len) * groups
            for g in range(groups):
                chosen = live & ((position & (groups - 1)) == g)
                bias = jnp.where(chosen, 0.0, LOW)
                yield jnp.concatenate([bias] * (GROUP // 8), axis=0)

        for pair in range(batch // 2):
            both = (2 * pair, 2 * pair + 1)
            queries = [
                jnp.concatenate(
                    [
                        heads_all[step_index, pl.ds(g * PER_KV * 4 + b, GROUP, stride=4), :]
                        for g in range(groups)
                    ],
                    axis=0,
                )
                for b in both
            ]
            query = jnp.concatenate(
                [
                    jnp.concatenate([queries[0], blank], axis=1),
                    jnp.concatenate([blank, queries[1]], axis=1),
                ],
                axis=0,
            ).astype(jnp.bfloat16)
            tops = [None] * (2 * groups)
            for tile in range(tiles):
                columns = slice(tile * width, (tile + 1) * width)
                key = jnp.concatenate([keys[b, columns, :] for b in both], axis=1)
                raw = lax.dot_general(query, key, NT, preferred_element_type=jnp.float32)
                biases = [bias for b in both for bias in mask(b, tile)]
                for place, bias in enumerate(biases):
                    rows = slice(place * GROUP, (place + 1) * GROUP)
                    masked = raw[rows, :] + bias
                    scores[pair, rows, columns] = masked
                    top = over_lanes(masked, jnp.maximum)
                    tops[place] = top if tile == 0 else jnp.maximum(tops[place], top)
            tops = [
                jnp.maximum(jnp.max(top, axis=1, keepdims=True), 0.5 * LOW) for top in tops
            ]
            sums = [None] * (2 * groups)
            mixed = jnp.zeros((2 * head_rows, 2 * HEAD_DIM), jnp.float32)
            for tile in range(tiles):
                columns = slice(tile * width, (tile + 1) * width)
                weights = []
                for place in range(2 * groups):
                    rows = slice(place * GROUP, (place + 1) * GROUP)
                    weight = jnp.exp2((scores[pair, rows, columns] - tops[place]) * power)
                    part_sum = over_lanes(weight, jnp.add)
                    sums[place] = part_sum if tile == 0 else sums[place] + part_sum
                    weights.append(weight.astype(jnp.bfloat16))
                value = jnp.concatenate([values[b, columns, :] for b in both], axis=1)
                mixed = mixed + jnp.dot(
                    jnp.concatenate(weights, axis=0), value, preferred_element_type=jnp.float32
                )
            for side, b in enumerate(both):
                mine = slice(side * groups, (side + 1) * groups)
                top = jnp.concatenate(tops[mine], axis=0) * score_scale
                total = jnp.concatenate(
                    [jnp.sum(piece, axis=1, keepdims=True) for piece in sums[mine]], axis=0
                )
                spread = jnp.where(lane == line, top, 0.0) + jnp.where(
                    lane == line + LANES // 2, total, 0.0
                )
                spread = jnp.sum(spread, axis=0, keepdims=True)
                own = mixed[
                    side * head_rows : (side + 1) * head_rows,
                    side * HEAD_DIM : (side + 1) * HEAD_DIM,
                ]
                each = head_rows // rows_each
                for piece in range(each):
                    slot = step_index * count + b * each + piece
                    merge_send[slot, 0:rows_each, :] = own[
                        piece * rows_each : (piece + 1) * rows_each, :
                    ]
                    merge_send[slot, rows_each : rows_each + 1, :] = spread
        for step in range(1, count):
            merge_copy(step_index, step).start()

    def attended_place():
        first = me * rows_each
        b = first // head_rows
        line = lax.rem(first, head_rows)
        return b, line

    def attended_copy(step_index, step):
        b, line = attended_place()
        return pltpu.make_async_remote_copy(
            src_ref=attended_own.at[step_index],
            dst_ref=attended.at[step_index, pl.ds(line, rows_each), b, :],
            send_sem=attended_send_sem.at[step_index],
            recv_sem=attended_sem.at[step_index],
            device_id=(peer(step), head),
            device_id_type=MESH,
        )

    def merge(step_index):
        wait_bytes(merge_arrived.at[step_index, pl.ds(1, count - 1)], merge_sem.at[step_index])
        b, line = attended_place()
        own = step_index * count + me
        pieces = [merge_send[own, 0:rows_each, :]]
        stats = [merge_send[own, rows_each : rows_each + 1, :]]
        for step in range(1, count):
            pieces.append(merge_arrived[step_index, step, 0:rows_each, :])
            stats.append(merge_arrived[step_index, step, rows_each : rows_each + 1, :])
        top = stats[0]
        for stat in stats[1:]:
            top = jnp.maximum(top, stat)
        lane = lax.broadcasted_iota(jnp.int32, (rows_each, LANES), 1)
        row = lax.broadcasted_iota(jnp.int32, (rows_each, LANES), 0)
        chosen = lane == line + row

        def to_column(values_row):
            spread = jnp.where(chosen, jnp.broadcast_to(values_row, (rows_each, LANES)), 0.0)
            return jnp.sum(spread, axis=1, keepdims=True)

        upper = lax.broadcasted_iota(jnp.int32, (1, LANES), 1) < LANES // 2
        numerator = jnp.zeros((rows_each, HEAD_DIM), jnp.float32)
        denominator_row = jnp.zeros((1, LANES), jnp.float32)
        for piece, stat in zip(pieces, stats):
            factor = jnp.exp(jnp.where(upper, stat - top, LOW))
            numerator = numerator + piece * to_column(factor)
            sums = jnp.concatenate([stat[:, LANES // 2 :], stat[:, : LANES // 2]], axis=1)
            denominator_row = denominator_row + sums * factor
        top_column = to_column(top)
        denominator = to_column(denominator_row)
        group = line // GROUP
        start = (group * PER_KV + lax.rem(line, GROUP)) * 4 + b
        query = heads_all[step_index, pl.ds(start, rows_each, stride=4), :]
        new_at = (group * PER_KV + GROUP) * 4 + b
        new_scores = []
        new_values = []
        for past in range(step_index + 1):
            new_key = heads_all[past, pl.ds(new_at, 1), :]
            new_values.append(heads_all[past, pl.ds(new_at + 4, 1), :])
            new_scores.append(jnp.sum(query * new_key, axis=1, keepdims=True) * score_scale)
        peak = top_column
        for new_score in new_scores:
            peak = jnp.maximum(peak, new_score)
        factor = jnp.exp(top_column - peak)
        denominator = denominator * factor
        numerator = numerator * factor
        for new_score, new_value in zip(new_scores, new_values):
            weight = jnp.exp(new_score - peak)
            denominator = denominator + weight
            numerator = numerator + weight * new_value
        attended_own[step_index] = numerator / denominator
        for step in range(1, count):
            attended_copy(step_index, step).start()
        for place in range(rows_each):
            attended[step_index, line + place, pl.ds(b, 1), :] = attended_own[
                step_index, place : place + 1, :
            ]

    def share_copy(step_index, step):
        other = lax.rem(head + step, head_count)
        return pltpu.make_async_remote_copy(
            src_ref=share.at[step_index],
            dst_ref=share_arrived.at[step_index, head],
            send_sem=share_send_sem.at[step_index],
            recv_sem=share_sem.at[step_index],
            device_id=(me, other),
            device_id_type=MESH,
        )

    def project(step_index):
        wait_bytes(attended_bytes(step_index), attended_sem.at[step_index])
        lines = jnp.concatenate(
            [
                attended[step_index, pl.ds(place, out_chunks, stride=4), :, :].reshape(
                    out_chunks * 8, LANES
                )
                for place in range(4)
            ],
            axis=1,
        ).astype(jnp.bfloat16)
        moved = jnp.dot(lines, perm[...], preferred_element_type=jnp.float32)
        by_phase[...] = moved.reshape(out_chunks, 8, WIDE)

        together = max(size for size in (4, 2, 1) if out_chunks % size == 0)

        def body(index, total):
            for place in range(together):
                chunk = index * together + place
                weights = jnp.concatenate(
                    [w_out[chunk, block] for block in range(depth // LANES)], axis=1
                )
                total = total + jnp.dot(
                    by_phase[chunk].astype(jnp.bfloat16),
                    weights,
                    preferred_element_type=jnp.float32,
                )
            return total

        blank = jnp.zeros((8, depth), jnp.float32)
        total = lax.fori_loop(0, out_chunks // together, body, blank)
        scaled = total[0:batch, :] * (out_scale[...] / code_norm)
        share[step_index] = scaled
        share_arrived[step_index, head] = scaled
        for step in range(1, head_count):
            share_copy(step_index, step).start()
        wait_bytes(share_arrived.at[step_index, pl.ds(0, head_count - 1)], share_sem.at[step_index])
        update = share_arrived[step_index, 0]
        for other in range(1, head_count):
            update = update + share_arrived[step_index, other]
        fresh = (hidden[...] + update).astype(jnp.bfloat16)
        hidden[...] = fresh.astype(jnp.float32)

    def attended_bytes(step_index):
        return merge_arrived.at[step_index, pl.ds(1, count - 1), 0:rows_each, :]

    begin_step(0)
    qkv.first_windows()
    outs.begin()
    pl.semaphore_wait(barrier, count - 1 + head_count - 1)
    for step in range(1, count):
        square_copy(0, step).start()

    def beside(chunk, step, rows):
        before = jnp.maximum(chunk - 1, 0)
        weights = jnp.concatenate([w_qkv[before, phase, rows, :] for phase in range(4)], axis=1)
        product = jnp.dot(normed[:, rows], weights, preferred_element_type=jnp.float32)
        accum[...] += product

    def qkv_step(chunk, carry):
        accum[...] = jnp.zeros_like(accum)
        qkv.chunk(chunk, beside)
        part[0, chunk - 1] = accum[0:batch, :]
        send_part(0, chunk - 1)
        return carry

    qkv.chunk(0)
    lax.fori_loop(1, chunks, qkv_step, 0)
    part[0, chunks - 1] = qkv_product(chunks - 1)[0:batch, :]
    send_part(0, chunks - 1)
    for b in range(batch):
        pltpu.make_async_copy(keys_hbm.at[b], keys.at[b], cache_sem.at[0, b]).start()
        pltpu.make_async_copy(values_hbm.at[b], values.at[b], cache_sem.at[1, b]).start()
    marks = [0, out_chunks * 3 // 16, out_chunks * 7 // 16, out_chunks * 12 // 16, out_chunks]
    outs.first_windows()
    outs.run(marks[0], marks[1])
    finish_heads(0)
    outs.run(marks[1], marks[2])
    attend(0)
    outs.run(marks[2], marks[3])
    merge(0)
    outs.run(marks[3], marks[4])
    project(0)

    for step_index in range(1, DECODE_STEPS):
        begin_step(step_index)
        for step in range(1, count):
            square_copy(step_index, step).start()

        together = max(size for size in (3, 2, 1) if chunks % size == 0)

        def again(index, carry):
            several = [index * together + place for place in range(together)]
            for chunk, product in zip(several, [qkv_product(chunk) for chunk in several]):
                part[step_index, chunk] = product[0:batch, :]
            for chunk in several:
                send_part(step_index, chunk)
            return carry

        lax.fori_loop(0, chunks // together, again, 0)
        finish_heads(step_index)
        attend(step_index)
        merge(step_index)
        project(step_index)

    out_ref[...] = hidden[...].astype(jnp.bfloat16)

    for step_index in range(DECODE_STEPS):
        others = pl.ds(1, count - 1)
        wait_bytes(square_all.at[step_index, others], square_send_sem.at[step_index])
        wait_bytes(merge_arrived.at[step_index, others], merge_send_sem.at[step_index])
        wait_bytes(attended_bytes(step_index), attended_send_sem.at[step_index])
        heads_away = share_arrived.at[step_index, pl.ds(0, head_count - 1)]
        wait_bytes(heads_away, share_send_sem.at[step_index])
        wait_part_sends(step_index)


def rope_tables(lengths, batch, step, phase):
    half = HEAD_DIM // 2
    row = lax.broadcasted_iota(jnp.int32, (8, LANES), 0)
    lane = lax.broadcasted_iota(jnp.int32, (8, LANES), 1)
    entry = 4 * (lane & (TILE_BYTES - 1)) + phase
    place = (entry & (half - 1)).astype(jnp.float32)
    freqs = jnp.exp(-(place * (2.0 / HEAD_DIM)) * math.log(rope_base))
    position = jnp.zeros((8, LANES), jnp.int32)
    for b in range(batch):
        position = jnp.where(row == b, lengths[b] + step, position)
    angle = position.astype(jnp.float32) * freqs
    sine = jnp.sin(angle)
    return jnp.cos(angle), jnp.where(entry < half, -sine, sine)


def padded_codes(codes):
    extra = -codes.shape[1] % LANES
    return jnp.pad(codes, ((0, 0), (0, extra))) if extra else codes


def shards(
    hidden_in,
    norm_gain,
    qkv_codes,
    qkv_scale,
    out_codes,
    out_scale,
    cache_keys,
    cache_values,
    lengths,
):
    count = lax.axis_size("seq")
    head_count = lax.axis_size("head")
    batch, depth = hidden_in.shape
    qkv_codes = padded_codes(qkv_codes)
    out_codes = padded_codes(out_codes)
    chunks = qkv_codes.shape[1] // LANES
    out_chunks = out_codes.shape[1] // LANES
    extra = chunks * WIDE - qkv_scale.shape[0]
    if extra:
        qkv_scale = jnp.pad(qkv_scale, (0, extra))
    groups = cache_keys.shape[2]
    cached = cache_keys.shape[1] * groups
    head_rows = groups * GROUP
    rows_each = batch * head_rows // count
    owners = -(-chunks // count)
    f32, bf16 = jnp.float32, jnp.bfloat16
    vmem = pl.BlockSpec(memory_space=pltpu.VMEM)
    hbm = pl.BlockSpec(memory_space=pl.ANY)
    steps = DECODE_STEPS
    dma = pltpu.SemaphoreType.DMA
    return pl.pallas_call(
        kernel,
        in_specs=[
            vmem, vmem, hbm, vmem, hbm, vmem, hbm, hbm,
            pl.BlockSpec(memory_space=pltpu.SMEM),
        ],
        out_specs=vmem,
        out_shape=jax.ShapeDtypeStruct((batch, depth), bf16),
        scratch_shapes=[
            pltpu.VMEM((chunks, 4, depth, LANES), bf16),
            pltpu.VMEM((out_chunks, depth // LANES, WIDE, LANES), bf16),
            pltpu.VMEM((DEPTH, depth, LANES), jnp.int32),
            pltpu.VMEM((2, depth, LANES), jnp.int32),
            pltpu.VMEM((DEPTH, depth, LANES), jnp.int32),
            pltpu.VMEM((2, depth, LANES), jnp.int32),
            pltpu.VMEM((batch, cached, HEAD_DIM), bf16),
            pltpu.VMEM((batch, cached, HEAD_DIM), bf16),
            pltpu.VMEM((steps, 4, 8, LANES), f32),
            pltpu.VMEM((steps, 4, 8, LANES), f32),
            pltpu.VMEM((WIDE, WIDE), bf16),
            pltpu.VMEM((2, LANES, LANES), bf16),
            pltpu.VMEM((16, depth), f32),
            pltpu.VMEM((16, depth), bf16),
            pltpu.VMEM((batch, depth), f32),
            pltpu.VMEM((16, WIDE), f32),
            pltpu.VMEM((steps, chunks, batch, WIDE), f32),
            pltpu.VMEM((16, WIDE), f32),
            pltpu.VMEM((owners, 8, WIDE), f32),
            pltpu.VMEM((steps, count, batch, LANES), f32),
            pltpu.VMEM((steps, owners, count - 1, batch, WIDE), f32),
            pltpu.VMEM((steps, chunks * 16, LANES), f32),
            pltpu.VMEM((batch // 2, 2 * head_rows, cached), f32),
            pltpu.VMEM((steps * count, rows_each + 1, LANES), f32),
            pltpu.VMEM((steps, count, rows_each + 1, LANES), f32),
            pltpu.VMEM((steps, head_rows, 8, LANES), f32),
            pltpu.VMEM((steps, rows_each, LANES), f32),
            pltpu.VMEM((out_chunks, 8, WIDE), f32),
            pltpu.VMEM((steps, batch, depth), f32),
            pltpu.VMEM((steps, head_count, batch, depth), f32),
            dma((DEPTH,)),
            dma((DEPTH,)),
            dma((2, batch)),
            dma((steps,)),
            dma((steps,)),
            dma((steps,)),
            dma((steps, owners)),
            dma((steps, owners)),
            dma((steps,)),
            dma((steps,)),
            dma((steps,)),
            dma((steps,)),
            dma((steps,)),
            dma((steps,)),
            dma((steps,)),
        ],
        compiler_params=pltpu.CompilerParams(
            collective_id=0, has_side_effects=True, vmem_limit_bytes=66_000_000
        ),
    )(
        hidden_in,
        norm_gain[None, :],
        qkv_codes,
        qkv_scale[None, :],
        out_codes,
        out_scale[None, :],
        cache_keys.reshape(batch, cached, HEAD_DIM),
        cache_values.reshape(batch, cached, HEAD_DIM),
        lengths,
    )


def solution(mesh):
    in_specs = (
        P(None, "seq"),
        P("seq"),
        P("seq", "head"),
        P("head"),
        P("seq", "head"),
        P("seq"),
        P(None, "seq", "head", None),
        P(None, "seq", "head", None),
        P(),
    )
    out_specs = P(None, "seq")
    return jax.shard_map(shards, mesh=mesh, in_specs=in_specs, out_specs=out_specs, check_vma=False)
```
